32 devices in a mesh: gz: 16 (over z, y, core), gy: 2 (over x).
Axes of the slice: x: 2, y: 2, z: 4, core: 2. Of those that a mesh axis runs over, the one named last changes fastest.
Arguments:
- estimate: float32 [256, 64, 512], P('gz', 'gy'), may hold values from 0.5 to 2
- measured: float32 [4, 256, 64, 512], P(None, 'gz', 'gy'), may hold values from 0.25 to 4
- psf_z: float32 [4, 31], replicated, may hold values from 0.1 to 1
- psf_y: float32 [4, 15], replicated, may hold values from 0.1 to 1
- psf_x: float32 [4, 15], replicated, may hold values from 0.1 to 1
- extents: int32 [4, 3], replicated, may hold values from 9 to 31, as said below
- order: int32 [4], replicated, may hold values from 0 to 3, each once
Outputs:
- updated: float32 [256, 64, 512], P('gz', 'gy')
The draws below stay inside these ranges and needn't reach their ends.
Inputs may be any that keep to these rules, and one draw needn't show every extreme that they name: `extents`: every extent is odd; along z it lies in 9 to 31, along y and x in 9 to 15; in every draw some view has extent 31 along z and some view has extent 15 along y.
All inputs are finite; a program needn't handle non-finite values.
Results may differ from the reference program's by a relative error of at most 0.0001.
Values sent between devices are 32-bit elements; how exact they have to be, the bound alone decides.
A program may use at most 64 MiB of HBM per device.

```python
import math
import jax
import jax.numpy as jnp
from jax import lax

NX = 512
V = 4
KZ = 31
KL = 15
NZ = 256
NY = 64


def draw_extents(key, part):
    keys = jax.random.split(jax.random.fold_in(key, 7), 5)
    radius_z = jax.random.randint(keys[0], (V,), 4, 16)
    radius_y = jax.random.randint(keys[1], (V,), 4, 8)
    radius_x = jax.random.randint(keys[2], (V,), 4, 8)
    views = jnp.arange(V, dtype=jnp.int32)
    pick_z = jax.random.randint(keys[3], (), 0, V)
    pick_y = jax.random.randint(keys[4], (), 0, V)
    radius_z = jnp.where(views == pick_z, 15, radius_z)
    radius_y = jnp.where(views == pick_y, 7, radius_y)
    radii = jnp.stack([radius_z, radius_y, radius_x], axis=1)
    return (2 * radii + 1).astype(jnp.int32)


def block_scale(own_key, dims, pieces, least, top_value):
    def one(axis_at, parts):
        heights = jax.random.uniform(jax.random.fold_in(jax.random.fold_in(own_key, 6), axis_at), (parts,), jnp.float32, least / len(pieces), top_value / len(pieces))
        return jnp.repeat(jnp.exp(heights), dims[axis_at] // parts).reshape((-1,) + (1,) * (len(dims) - axis_at - 1))

    level = one(*pieces[0])
    for cut in pieces[1:]:
        level = level * one(*cut)
    return level


def setup_inputs(seed: int = 0) -> dict:
    streams_of = jax.random.split(jax.random.key(seed), 8)
    return {
        "estimate": jnp.clip(jnp.exp(math.log(2.0) - 1.3862944 * jax.random.uniform(streams_of[0], (NZ, NY, NX), jnp.float32) ** block_scale(streams_of[0], (NZ, NY, NX), ((0, 16), (1, 2)), -0.2, 0.2)), 0.5, 2.0),
        "measured": jnp.clip(jnp.exp(math.log(4.0) - 2.7725887 * jax.random.uniform(streams_of[1], (V, NZ, NY, NX), jnp.float32) ** block_scale(streams_of[1], (V, NZ, NY, NX), ((1, 16), (2, 2)), -0.2, 0.2)), 0.25, 4.0),
        "psf_z": jnp.clip(jnp.exp(jax.random.uniform(streams_of[2], (V, KZ), jnp.float32, math.log(0.1), math.log(1.0))), 0.1, 1.0),
        "psf_y": jnp.clip(jnp.exp(jax.random.uniform(streams_of[3], (V, KL), jnp.float32, math.log(0.1), math.log(1.0))), 0.1, 1.0),
        "psf_x": jnp.clip(jnp.exp(jax.random.uniform(streams_of[4], (V, KL), jnp.float32, math.log(0.1), math.log(1.0))), 0.1, 1.0),
        "extents": draw_extents(jax.random.fold_in(streams_of[7], 71), 0),
        "order": jax.random.permutation(streams_of[6], V).astype(jnp.int32),
    }


def line_taps(profile, reach_cells, tap_reach):
    offsets = jnp.arange(2 * tap_reach + 1, dtype=jnp.int32) - tap_reach
    kept = jnp.where(jnp.abs(offsets) <= reach_cells, profile, jnp.zeros_like(profile))
    return kept / jnp.sum(kept)


def pad_axis(field, along_axis, tap_reach):
    widths = [(0, 0), (0, 0), (0, 0)]
    widths[along_axis] = (tap_reach, tap_reach)
    return jnp.pad(field, widths)


def correlate_padded(padded, weights, along_axis, tap_reach, length, flipped):
    total = None
    for offset in range(2 * tap_reach + 1):
        start = 2 * tap_reach - offset if flipped else offset
        piece = lax.slice_in_dim(padded, start, start + length, axis=along_axis)
        term = weights[offset] * piece
        total = term if total is None else total + term
    return total


def blur(field, weights_z, weights_y, weights_x, flipped):
    result = correlate_padded(pad_axis(field, 0, 15), weights_z, 0, 15, field.shape[0], flipped)
    result = correlate_padded(pad_axis(result, 1, 7), weights_y, 1, 7, field.shape[1], flipped)
    result = correlate_padded(pad_axis(result, 2, 7), weights_x, 2, 7, field.shape[2], flipped)
    return result


def reference(estimate, measured, psf_z, psf_y, psf_x, extents, order):
    current = estimate
    for position in range(V):
        view = order[position]
        radii = (extents[view] - 1) // 2
        weights_z = line_taps(psf_z[view], radii[0], 15)
        weights_y = line_taps(psf_y[view], radii[1], 7)
        weights_x = line_taps(psf_x[view], radii[2], 7)
        blurred = blur(current, weights_z, weights_y, weights_x, False)
        ratio = measured[view] / blurred
        current = current * blur(ratio, weights_z, weights_y, weights_x, True)
    return current
```

```python
import functools
import jax
import jax.numpy as jnp
from jax import lax
from jax.experimental import pallas as pl
from jax.experimental.pallas import tpu as pltpu
from jax.sharding import PartitionSpec as P

MESH = pl.DeviceIdType.MESH
RZ = 15
RL = 7
LANES = 128


def with_halo(value, sides, width):
    for axis, dim in sides:
        size, length = (lax.axis_size(axis), value.shape[dim])
        up = [(i, (i + 1) % size) for i in range(size - 1)]
        down = [(j, i) for i, j in up]
        last = lax.slice_in_dim(value, length - width, length, axis=dim)
        initial = lax.slice_in_dim(value, 0, width, axis=dim)
        before = lax.ppermute(last, axis, up)
        after = lax.ppermute(initial, axis, down)
        value = jnp.concatenate([before, value, after], axis=dim)
    return value


def line_taps(profile, reach_cells, tap_reach):
    offsets = jnp.arange(2 * tap_reach + 1, dtype=jnp.int32) - tap_reach
    kept = jnp.where(jnp.abs(offsets) <= reach_cells, profile, jnp.zeros_like(profile))
    return kept / jnp.sum(kept)


def correlate_padded(padded, weights, along_axis, tap_reach, length, flipped):
    total = None
    for offset in range(2 * tap_reach + 1):
        start = 2 * tap_reach - offset if flipped else offset
        piece = lax.slice_in_dim(padded, start, start + length, axis=along_axis)
        term = weights[offset] * piece
        total = term if total is None else total + term
    return total


def blur(field, weights_z, weights_y, weights_x, flipped):
    padded = with_halo(field, (("gz", 0),), RZ)
    result = correlate_padded(padded, weights_z, 0, RZ, field.shape[0], flipped)
    widened = with_halo(result, (("gy", 1),), RL)
    result = correlate_padded(widened, weights_y, 1, RL, field.shape[1], flipped)
    result = jnp.pad(result, ((0, 0), (0, 0), (RL, RL)))
    return correlate_padded(result, weights_x, 2, RL, field.shape[2], flipped)


def general(estimate, measured, psf_z, psf_y, psf_x, extents, order):
    current = estimate
    for position in range(measured.shape[0]):
        view = order[position]
        radii = (extents[view] - 1) // 2
        weights_z = line_taps(psf_z[view], radii[0], RZ)
        weights_y = line_taps(psf_y[view], radii[1], RL)
        weights_x = line_taps(psf_x[view], radii[2], RL)
        recorded = lax.dynamic_index_in_dim(measured, view, 0, keepdims=False)
        blurred = blur(current, weights_z, weights_y, weights_x, False)
        ratio = recorded / blurred
        current = current * blur(ratio, weights_z, weights_y, weights_x, True)
    return current


def place():
    g = lax.axis_index("gz")
    w = lax.axis_index("gy")
    return g // 4, (g // 2) % 2, g % 2, w


def slab_of(a, w):
    return 2 * a + lax.rem(w + a, 2)


def group_peers():
    h, a, c, w = place()
    peers = []
    for k in range(1, 8):
        da, dc, dw = k // 4, (k // 2) % 2, k % 2
        device = (4 * h + 2 * lax.rem(a + da, 2) + lax.rem(c + dc, 2), lax.rem(w + dw, 2))
        peers.append(device)
    return peers


def spread_kernel(nz, ny, back, n, *refs):
    srcs, dsts = refs[:n], refs[n:2 * n]
    send, recv, local = refs[2 * n:]
    h, a, c, w = place()
    barrier = pltpu.get_barrier_semaphore()
    for device in group_peers():
        pl.semaphore_signal(barrier, inc=1, device_id=device, device_id_type=MESH)
    pl.semaphore_wait(barrier, 7)
    for phase in ("start", "wait"):
        for i in range(n):
            for k in range(4):
                da, dw = k // 2, k % 2
                if not back:
                    ta, tw = lax.rem(c + da, 2), lax.rem(w + dw, 2)
                    device = (4 * h + 2 * ta + a, tw)
                    x0 = pl.multiple_of(LANES * slab_of(ta, tw), LANES)
                    src = srcs[i].at[:, :, pl.ds(x0, LANES)]
                    dst = dsts[i].at[pl.ds(nz * c, nz), pl.ds(pl.multiple_of(ny * w, 8), ny), :]
                    mine = jnp.logical_and(c == a, jnp.logical_and(ta == a, tw == w))
                else:
                    tc, tw = lax.rem(a + da, 2), lax.rem(w + dw, 2)
                    device = (4 * h + 2 * c + tc, tw)
                    x0 = pl.multiple_of(LANES * slab_of(a, w), LANES)
                    src = srcs[i].at[pl.ds(nz * tc, nz), pl.ds(pl.multiple_of(ny * tw, 8), ny), :]
                    dst = dsts[i].at[:, :, pl.ds(x0, LANES)]
                    mine = jnp.logical_and(c == a, jnp.logical_and(tc == c, tw == w))
                remote = pltpu.make_async_remote_copy(
                    src_ref=src, dst_ref=dst, send_sem=send.at[i, k], recv_sem=recv.at[i, k],
                    device_id=device, device_id_type=MESH)
                if phase == "start":
                    @pl.when(mine)
                    def _():
                        pltpu.make_async_copy(src, dst, local.at[i]).start()

                    @pl.when(jnp.logical_not(mine))
                    def _():
                        remote.start()
                else:
                    @pl.when(mine)
                    def _():
                        pltpu.make_async_copy(src, dst, local.at[i]).wait()

                    @pl.when(jnp.logical_not(mine))
                    def _():
                        remote.wait()


def spread(arrays, nz, ny, nx, back, cid):
    n = len(arrays)
    shape = (nz, ny, nx) if back else (2 * nz, 2 * ny, LANES)
    out = pl.pallas_call(
        functools.partial(spread_kernel, nz, ny, back, n),
        out_shape=[jax.ShapeDtypeStruct(shape, jnp.float32)] * n,
        in_specs=[pl.BlockSpec(memory_space=pl.ANY)] * n,
        out_specs=[pl.BlockSpec(memory_space=pl.ANY)] * n,
        scratch_shapes=[
            pltpu.SemaphoreType.DMA((n, 4)),
            pltpu.SemaphoreType.DMA((n, 4)),
            pltpu.SemaphoreType.DMA((n,)),
        ],
        compiler_params=pltpu.CompilerParams(collective_id=cid, has_side_effects=True),
    )(*arrays)
    return out


def split(value):
    hi = value.astype(jnp.bfloat16)
    lo = (value - hi.astype(jnp.float32)).astype(jnp.bfloat16)
    return hi, lo


CHUNKS = 4


def blur_kernel(divide, chain, f, other, wz, ym, xm, xe, out,
                below, above, zb, pack_l, pack_r, got_l, got_r, zs, zr, xs, xr):
    planes, rows, _ = f.shape
    h, a, c, w = place()
    zi = 2 * h + c
    s = slab_of(a, w)
    has_dn, has_up = zi > 0, zi < chain - 1
    has_l, has_r = s > 0, s < 3

    def z_dev(i):
        return (4 * (i // 2) + 2 * a + lax.rem(i, 2), w)

    def x_dev(i):
        b = i // 2
        return (4 * h + 2 * b + c, lax.rem(i + b, 2))

    up, dn = z_dev(lax.rem(zi + 1, chain)), z_dev(lax.rem(zi + chain - 1, chain))
    lf, rt = x_dev(lax.rem(s + 3, 4)), x_dev(lax.rem(s + 1, 4))

    barrier = pltpu.get_barrier_semaphore()
    for there, device in ((has_up, up), (has_dn, dn), (has_l, lf), (has_r, rt)):
        @pl.when(there)
        def _():
            pl.semaphore_signal(barrier, inc=1, device_id=device, device_id_type=MESH)
    peers = sum(there.astype(jnp.int32) for there in (has_up, has_dn, has_l, has_r))
    pl.semaphore_wait(barrier, peers)

    part = rows // CHUNKS

    def z_copy(side, j):
        ys = pl.ds(j * part, part)
        if side == 0:
            return pltpu.make_async_remote_copy(
                src_ref=f.at[pl.ds(planes - RZ, RZ), ys, :], dst_ref=below.at[:, ys, :],
                send_sem=zs.at[0, j], recv_sem=zr.at[0, j], device_id=up, device_id_type=MESH)
        return pltpu.make_async_remote_copy(
            src_ref=f.at[pl.ds(0, RZ), ys, :], dst_ref=above.at[:, ys, :],
            send_sem=zs.at[1, j], recv_sem=zr.at[1, j], device_id=dn, device_id_type=MESH)

    def x_copy(side):
        if side == 0:
            return pltpu.make_async_remote_copy(
                src_ref=pack_r, dst_ref=got_l,
                send_sem=xs.at[0], recv_sem=xr.at[0], device_id=rt, device_id_type=MESH)
        return pltpu.make_async_remote_copy(
            src_ref=pack_l, dst_ref=got_r,
            send_sem=xs.at[1], recv_sem=xr.at[1], device_id=lf, device_id_type=MESH)

    for j in range(CHUNKS):
        @pl.when(has_up)
        def _():
            z_copy(0, j).start()

        @pl.when(has_dn)
        def _():
            z_copy(1, j).start()

    @pl.when(jnp.logical_not(has_dn))
    def _():
        below[...] = jnp.zeros_like(below)

    @pl.when(jnp.logical_not(has_up))
    def _():
        above[...] = jnp.zeros_like(above)

    @pl.when(jnp.logical_not(has_l))
    def _():
        got_l[...] = jnp.zeros_like(got_l)

    @pl.when(jnp.logical_not(has_r))
    def _():
        got_r[...] = jnp.zeros_like(got_r)

    half = 16

    def z_tile(t, carry):
        ys = pl.ds(pl.multiple_of(8 * t, 8), 8)
        taps = [wz[k] for k in range(2 * RZ + 1)]
        for first in range(0, planes, half):
            acc = [None] * half
            for p in range(first, first + half + 2 * RZ):
                if p < RZ:
                    v = below[p, ys, :]
                elif p < RZ + planes:
                    v = f[p - RZ, ys, :]
                else:
                    v = above[p - RZ - planes, ys, :]
                for o in range(half):
                    k = p - first - o
                    if 0 <= k <= 2 * RZ:
                        term = taps[k] * v
                        acc[o] = term if acc[o] is None else acc[o] + term
            for o in range(half):
                zb[first + o, ys, :] = acc[o]
        return carry

    for j in range(CHUNKS):
        @pl.when(has_dn)
        def _():
            z_copy(0, j).wait_recv()

        @pl.when(has_up)
        def _():
            z_copy(1, j).wait_recv()

        lax.fori_loop(j * part // 8, (j + 1) * part // 8, z_tile, 0)

    for j in range(CHUNKS):
        @pl.when(has_up)
        def _():
            z_copy(0, j).wait_send()

        @pl.when(has_dn)
        def _():
            z_copy(1, j).wait_send()

    lane = lax.broadcasted_iota(jnp.int32, (rows, LANES), 1)
    per = LANES // 8

    for q in range(planes // per):
        packed_l = packed_r = None
        for k in range(0, per, 2):
            p = q * per + k
            his, los = zip(*(split(zb[p + i]) for i in range(2)))
            hi = jnp.concatenate(his, axis=1)
            lo = jnp.concatenate(los, axis=1)
            got = jnp.dot(ym[...], jnp.concatenate([hi, lo, hi, lo], axis=0),
                          preferred_element_type=jnp.float32)
            for i in range(2):
                value = got[:, i * LANES:(i + 1) * LANES]
                zb[p + i] = value
                at = 8 * (k + i)
                left = value if at == 0 else pltpu.roll(value, at, 1)
                right = pltpu.roll(value, (at + 8) % LANES, 1) if at + 8 < LANES else value
                if packed_l is None:
                    packed_l, packed_r = left, right
                else:
                    packed_l = jnp.where(lane >= at, left, packed_l)
                    packed_r = jnp.where(lane >= at, right, packed_r)
        pack_l[q] = packed_l
        pack_r[q] = packed_r

    @pl.when(has_r)
    def _():
        x_copy(0).start()

    @pl.when(has_l)
    def _():
        x_copy(1).start()

    step = 4
    for p in range(0, planes, step):
        hi, lo = split(zb[p:p + step].reshape(step * rows, LANES))
        got = jnp.dot(jnp.concatenate([hi, lo], axis=1), xm[...], preferred_element_type=jnp.float32)
        zb[p:p + step] = (got[:, :LANES] + got[:, LANES:]).reshape(step, rows, LANES)

    @pl.when(has_l)
    def _():
        x_copy(0).wait_recv()

    @pl.when(has_r)
    def _():
        x_copy(1).wait_recv()

    for p in range(0, planes, step):
        edges = []
        for i in range(step):
            q, k = divmod(p + i, per)
            left, right = got_l[q], got_r[q]
            at = 8 * k
            left = left if at == 0 else pltpu.roll(left, LANES - at, 1)
            right = right if at == 8 else pltpu.roll(right, (LANES - at + 8) % LANES, 1)
            edges.append(jnp.where(lane < 8, left, right))
        hi, lo = split(jnp.concatenate(edges, axis=0))
        got = jnp.dot(jnp.concatenate([hi, lo], axis=1), xe[...], preferred_element_type=jnp.float32)
        value = zb[p:p + step] + (got[:, :LANES] + got[:, LANES:]).reshape(step, rows, LANES)
        if divide:
            out[p:p + step] = other[p:p + step] / value
        else:
            out[p:p + step] = other[p:p + step] * value

    @pl.when(has_r)
    def _():
        x_copy(0).wait_send()

    @pl.when(has_l)
    def _():
        x_copy(1).wait_send()


def slab_blur(f, other, wz, ym, xm, xe, divide, chain):
    planes, rows, _ = f.shape
    vmem = pl.BlockSpec(memory_space=pltpu.VMEM)
    packs = pltpu.VMEM((planes * 8 // LANES, rows, LANES), jnp.float32)
    return pl.pallas_call(
        functools.partial(blur_kernel, divide, chain),
        out_shape=jax.ShapeDtypeStruct(f.shape, jnp.float32),
        in_specs=[vmem] * 6,
        out_specs=vmem,
        scratch_shapes=[
            pltpu.VMEM((RZ, rows, LANES), jnp.float32),
            pltpu.VMEM((RZ, rows, LANES), jnp.float32),
            pltpu.VMEM((planes, rows, LANES), jnp.float32),
            packs, packs, packs, packs,
            pltpu.SemaphoreType.DMA((2, CHUNKS)),
            pltpu.SemaphoreType.DMA((2, CHUNKS)),
            pltpu.SemaphoreType.DMA((2,)),
            pltpu.SemaphoreType.DMA((2,)),
        ],
        compiler_params=pltpu.CompilerParams(
            collective_id=3 if divide else 4, has_side_effects=True),
    )(f, other, wz, ym, xm, xe)


def halves(value):
    hi = lax.reduce_precision(value, 8, 7)
    return hi.astype(jnp.bfloat16), (value - hi).astype(jnp.bfloat16)


def band(weights, source, target, reach):
    which = source[:, None] - target[None, :] + reach
    total = jnp.zeros((weights.shape[0],) + which.shape, jnp.float32)
    for k in range(2 * reach + 1):
        total = jnp.where(which == k, weights[:, k][:, None, None], total)
    return total


def all_taps(profiles, radii, reach):
    offsets = jnp.abs(jnp.arange(2 * reach + 1, dtype=jnp.int32) - reach)
    kept = jnp.where(offsets[None] <= radii[:, None], profiles, 0.0)
    taps = kept / jnp.sum(kept, axis=1, keepdims=True)
    return jnp.stack([taps, taps[:, ::-1]], axis=1).reshape(-1, 2 * reach + 1)


def slabs(chain, estimate, measured, psf_z, psf_y, psf_x, extents, order):
    views, nz, ny, nx = measured.shape
    rows = 2 * ny
    radii = ((extents - 1) // 2)[order]
    wz = all_taps(psf_z[order], radii[:, 0], RZ)
    wy = all_taps(psf_y[order], radii[:, 1], RL)
    wx = all_taps(psf_x[order], radii[:, 2], RL)
    wz = jnp.broadcast_to(wz[:, :, None, None], wz.shape + (8, LANES))
    cells = jnp.arange(rows, dtype=jnp.int32)
    hi, lo = halves(band(wy, cells, cells, RL).swapaxes(1, 2))
    ym = jnp.concatenate([hi, hi, lo, lo], axis=2)
    cells = jnp.arange(LANES, dtype=jnp.int32)
    hi, lo = halves(band(wx, cells, cells, RL))
    xm = jnp.concatenate([jnp.concatenate([hi, lo], axis=2)] * 2, axis=1)
    edge = jnp.where(cells < 8, cells - 8, jnp.where(cells < 16, LANES - 8 + cells, -4 * LANES))
    hi, lo = halves(band(wx, edge, cells, RL))
    xe = jnp.concatenate([jnp.concatenate([hi, lo], axis=2)] * 2, axis=1)
    recorded = [lax.dynamic_index_in_dim(measured, order[p], 0, keepdims=False) for p in range(views)]
    moved = spread([estimate] + recorded, nz, ny, nx, False, 1)
    current = moved[0]
    for p in range(views):
        i = 2 * p
        ratio = slab_blur(current, moved[1 + p], wz[i], ym[i], xm[i], xe[i], True, chain)
        i = i + 1
        current = slab_blur(ratio, current, wz[i], ym[i], xm[i], xe[i], False, chain)
    return spread([current], nz, ny, nx, True, 2)[0]


def on_device(estimate, measured, psf_z, psf_y, psf_x, extents, order):
    n_z, n_y = lax.axis_size("gz"), lax.axis_size("gy")
    nz, ny, nx = estimate.shape
    fits = n_y == 2 and n_z % 4 == 0 and nx == 4 * LANES and nz == 16 and 2 * ny == 64
    if fits:
        return slabs(n_z // 2, estimate, measured, psf_z, psf_y, psf_x, extents, order)
    return general(estimate, measured, psf_z, psf_y, psf_x, extents, order)


def solution(mesh):
    return jax.shard_map(
        on_device,
        mesh=mesh,
        in_specs=(P("gz", "gy", None), P(None, "gz", "gy", None), P(), P(), P(), P(), P()),
        out_specs=P("gz", "gy", None),
        check_vma=False,
    )
```

```python
import functools
import jax
import jax.numpy as jnp
from jax import lax
from jax.experimental import pallas as pl
from jax.experimental.pallas import tpu as pltpu
from jax.sharding import PartitionSpec as P

MESH = pl.DeviceIdType.MESH
RZ = 15
RL = 7
LANES = 128


def with_halo(value, sides, width):
    for axis, dim in sides:
        size, length = (lax.axis_size(axis), value.shape[dim])
        up = [(i, (i + 1) % size) for i in range(size - 1)]
        down = [(j, i) for i, j in up]
        last = lax.slice_in_dim(value, length - width, length, axis=dim)
        initial = lax.slice_in_dim(value, 0, width, axis=dim)
        before = lax.ppermute(last, axis, up)
        after = lax.ppermute(initial, axis, down)
        value = jnp.concatenate([before, value, after], axis=dim)
    return value


def line_taps(profile, reach_cells, tap_reach):
    offsets = jnp.arange(2 * tap_reach + 1, dtype=jnp.int32) - tap_reach
    kept = jnp.where(jnp.abs(offsets) <= reach_cells, profile, jnp.zeros_like(profile))
    return kept / jnp.sum(kept)


def correlate_padded(padded, weights, along_axis, tap_reach, length, flipped):
    total = None
    for offset in range(2 * tap_reach + 1):
        start = 2 * tap_reach - offset if flipped else offset
        piece = lax.slice_in_dim(padded, start, start + length, axis=along_axis)
        term = weights[offset] * piece
        total = term if total is None else total + term
    return total


def blur(field, weights_z, weights_y, weights_x, flipped):
    padded = with_halo(field, (("gz", 0),), RZ)
    result = correlate_padded(padded, weights_z, 0, RZ, field.shape[0], flipped)
    widened = with_halo(result, (("gy", 1),), RL)
    result = correlate_padded(widened, weights_y, 1, RL, field.shape[1], flipped)
    result = jnp.pad(result, ((0, 0), (0, 0), (RL, RL)))
    return correlate_padded(result, weights_x, 2, RL, field.shape[2], flipped)


def general(estimate, measured, psf_z, psf_y, psf_x, extents, order):
    current = estimate
    for position in range(measured.shape[0]):
        view = order[position]
        radii = (extents[view] - 1) // 2
        weights_z = line_taps(psf_z[view], radii[0], RZ)
        weights_y = line_taps(psf_y[view], radii[1], RL)
        weights_x = line_taps(psf_x[view], radii[2], RL)
        recorded = lax.dynamic_index_in_dim(measured, view, 0, keepdims=False)
        blurred = blur(current, weights_z, weights_y, weights_x, False)
        ratio = recorded / blurred
        current = current * blur(ratio, weights_z, weights_y, weights_x, True)
    return current


def place():
    g = lax.axis_index("gz")
    w = lax.axis_index("gy")
    return g // 4, (g // 2) % 2, g % 2, w


def slab_of(a, w):
    return 2 * a + lax.rem(w + a, 2)


def group_peers():
    h, a, c, w = place()
    peers = []
    for k in range(1, 8):
        da, dc, dw = k // 4, (k // 2) % 2, k % 2
        device = (4 * h + 2 * lax.rem(a + da, 2) + lax.rem(c + dc, 2), lax.rem(w + dw, 2))
        peers.append(device)
    return peers


def spread_kernel(nz, ny, back, srcs, dst_ref, send, recv, local, between=None):
    h, a, c, w = place()
    barrier = pltpu.get_barrier_semaphore()
    for device in group_peers():
        pl.semaphore_signal(barrier, inc=1, device_id=device, device_id_type=MESH)
    pl.semaphore_wait(barrier, 7)
    for phase in ("start", "wait"):
        for k in range(4):
            da, dw = k // 2, k % 2
            if not back:
                ta, tw = lax.rem(c + da, 2), lax.rem(w + dw, 2)
                device = (4 * h + 2 * ta + a, tw)
                x0 = pl.multiple_of(LANES * slab_of(ta, tw), LANES)
                src = srcs.at[:, :, pl.ds(x0, LANES)]
                dst = dst_ref.at[pl.ds(nz * c, nz), pl.ds(pl.multiple_of(ny * w, 8), ny), :]
            else:
                tc, tw = lax.rem(a + da, 2), lax.rem(w + dw, 2)
                device = (4 * h + 2 * c + tc, tw)
                x0 = pl.multiple_of(LANES * slab_of(a, w), LANES)
                src = srcs.at[pl.ds(nz * tc, nz), pl.ds(pl.multiple_of(ny * tw, 8), ny), :]
                dst = dst_ref.at[:, :, pl.ds(x0, LANES)]
            remote = pltpu.make_async_remote_copy(
                src_ref=src, dst_ref=dst, send_sem=send.at[k], recv_sem=recv.at[k],
                device_id=device, device_id_type=MESH)
            if k:
                if phase == "start":
                    remote.start()
                else:
                    remote.wait()
                continue
            here = pltpu.make_async_copy(src, dst, local)
            if phase == "start":
                @pl.when(c == a)
                def _():
                    here.start()

                @pl.when(c != a)
                def _():
                    remote.start()
            else:
                @pl.when(c == a)
                def _():
                    here.wait()

                @pl.when(c != a)
                def _():
                    remote.wait()
        if phase == "start" and between is not None:
            between()


SPREAD_SEMS = [
    pltpu.SemaphoreType.DMA((4,)),
    pltpu.SemaphoreType.DMA((4,)),
    pltpu.SemaphoreType.DMA,
]


def back_kernel(nz, ny, src, dst, send, recv, local):
    spread_kernel(nz, ny, True, src, dst, send, recv, local)


def gather_back(current, nz, ny, nx):
    return pl.pallas_call(
        functools.partial(back_kernel, nz, ny),
        out_shape=jax.ShapeDtypeStruct((nz, ny, nx), jnp.float32),
        in_specs=[pl.BlockSpec(memory_space=pl.ANY)],
        out_specs=pl.BlockSpec(memory_space=pl.ANY),
        scratch_shapes=SPREAD_SEMS,
        compiler_params=pltpu.CompilerParams(collective_id=2, has_side_effects=True),
    )(current)


def taps_of(profile, view, radius, reach):
    kept = []
    for k in range(2 * reach + 1):
        value = jnp.full((8, LANES), profile[view, k], jnp.float32)
        kept.append(jnp.where(abs(k - reach) <= radius, value, jnp.zeros_like(value)))
    total = kept[0]
    for value in kept[1:]:
        total = total + value
    return [value / total for value in kept]


def band(taps, which):
    total = jnp.zeros(which.shape, jnp.float32)
    for k, tap in enumerate(taps):
        total = jnp.where(which == k, tap[0:1, :], total)
    return split(total)


def first_kernel(nz, ny, views, est, psf_z, psf_y, psf_x, extents, order, *refs):
    n = 2 * views
    dst, wz, ym, xm, xe = refs[0], refs[1:1 + n], refs[1 + n:1 + 2 * n], refs[1 + 2 * n:1 + 3 * n], refs[1 + 3 * n:1 + 4 * n]
    send, recv, local = refs[1 + 4 * n:]
    rows = 2 * ny

    def build():
        def iota(shape, dim):
            return lax.broadcasted_iota(jnp.int32, shape, dim)

        y_which = lax.rem(iota((rows, LANES), 1), rows) - iota((rows, LANES), 0) + RL
        x_which = iota((LANES, LANES), 0) - iota((LANES, LANES), 1) + RL
        r = iota((16, LANES), 0)
        e_which = jnp.where(r < 8, r - 8, r + (LANES - 8)) - iota((16, LANES), 1) + RL
        for p in range(views):
            view = order[p]
            tz = taps_of(psf_z, view, (extents[view, 0] - 1) // 2, RZ)
            ty = taps_of(psf_y, view, (extents[view, 1] - 1) // 2, RL)
            tx = taps_of(psf_x, view, (extents[view, 2] - 1) // 2, RL)
            for i in (2 * p, 2 * p + 1):
                for k in range(2 * RZ + 1):
                    wz[i][k] = tz[k]
                hi, lo = band(ty, y_which)
                ym[i][:, :LANES] = hi
                ym[i][:, LANES:] = lo
                hi, lo = band(tx, x_which)
                for top in (0, LANES):
                    xm[i][top:top + LANES, :LANES] = hi
                    xm[i][top:top + LANES, LANES:] = lo
                hi, lo = band(tx, e_which)
                xe[i][...] = jnp.zeros_like(xe[i])
                for top in (0, LANES):
                    xe[i][top:top + 16, :LANES] = hi
                    xe[i][top:top + 16, LANES:] = lo
                tz, ty, tx = tz[::-1], ty[::-1], tx[::-1]

    spread_kernel(nz, ny, False, est, dst, send, recv, local, build)


def spread_first(estimate, psf_z, psf_y, psf_x, extents, order):
    nz, ny, nx = estimate.shape
    views = order.shape[0]
    n = 2 * views
    smem = pl.BlockSpec(memory_space=pltpu.SMEM)
    vmem = pl.BlockSpec(memory_space=pltpu.VMEM)
    like = jax.ShapeDtypeStruct
    out = pl.pallas_call(
        functools.partial(first_kernel, nz, ny, views),
        out_shape=[like((2 * nz, 2 * ny, LANES), jnp.float32)]
        + [like((2 * RZ + 1, 8, LANES), jnp.float32)] * n
        + [like((2 * ny, 2 * LANES), jnp.bfloat16)] * n
        + [like((2 * LANES, 2 * LANES), jnp.bfloat16)] * (2 * n),
        in_specs=[pl.BlockSpec(memory_space=pl.ANY)] + [smem] * 5,
        out_specs=[pl.BlockSpec(memory_space=pl.ANY)] + [vmem] * (4 * n),
        scratch_shapes=SPREAD_SEMS,
        compiler_params=pltpu.CompilerParams(collective_id=1, has_side_effects=True),
    )(estimate, psf_z, psf_y, psf_x, extents, order)
    return out[0], [out[1 + i::n][:4] for i in range(n)]


def split(value):
    hi = value.astype(jnp.bfloat16)
    lo = (value - hi.astype(jnp.float32)).astype(jnp.bfloat16)
    return hi, lo


CHUNKS = 4


def blur_kernel(kind, chain, *refs):
    divide = kind in (0, 2)
    refs = list(refs)
    f = refs.pop(0)
    other = refs.pop(0) if kind else None
    wz, ym, xm, xe = [refs.pop(0) for _ in range(4)]
    if kind < 3:
        view, measured = refs.pop(0), refs.pop(0)
    out = refs.pop(0)
    if kind == 1:
        moved = refs.pop(0)
    below, above, zb, pack_l, pack_r, got_l, got_r, zs, zr, xs, xr = refs[:11]
    refs = refs[11:]
    if kind < 3:
        stage, chosen, bs, br, bl = refs[:5]
        if kind != 1:
            moved = refs[5]
        nb = chosen.shape[0]
        ny = chosen.shape[1]
        nz = measured.shape[1]
    planes, rows, _ = f.shape
    h, a, c, w = place()
    zi = 2 * h + c
    s = slab_of(a, w)
    has_dn, has_up = zi > 0, zi < chain - 1
    has_l, has_r = s > 0, s < 3

    def z_dev(i):
        return (4 * (i // 2) + 2 * a + lax.rem(i, 2), w)

    def x_dev(i):
        b = i // 2
        return (4 * h + 2 * b + c, lax.rem(i + b, 2))

    up, dn = z_dev(lax.rem(zi + 1, chain)), z_dev(lax.rem(zi + chain - 1, chain))
    lf, rt = x_dev(lax.rem(s + 3, 4)), x_dev(lax.rem(s + 1, 4))

    barrier = pltpu.get_barrier_semaphore()
    greet = [(has_up, up), (has_dn, dn), (has_l, lf), (has_r, rt)]
    for there, device in greet:
        @pl.when(there)
        def _():
            pl.semaphore_signal(barrier, inc=1, device_id=device, device_id_type=MESH)
    peers = sum(there.astype(jnp.int32) for there, _ in greet)
    if kind < 3:
        for k in range(4):
            device = (4 * h + 2 * c + lax.rem(a + k // 2, 2), lax.rem(w + k % 2, 2))
            if k:
                pl.semaphore_signal(barrier, inc=1, device_id=device, device_id_type=MESH)
            else:
                @pl.when(c != a)
                def _():
                    pl.semaphore_signal(barrier, inc=1, device_id=device, device_id_type=MESH)
        peers = peers + 3 + (c != a).astype(jnp.int32)
        start = nz // 2 if kind == 2 else 0
        fetch = pltpu.make_async_copy(measured.at[:, pl.ds(start, nb)], stage, bl)
        fetch.start()
    pl.semaphore_wait(barrier, peers)

    part = rows // CHUNKS

    def z_copy(side, j):
        ys = pl.ds(j * part, part)
        if side == 0:
            return pltpu.make_async_remote_copy(
                src_ref=f.at[pl.ds(planes - RZ, RZ), ys, :], dst_ref=below.at[:, ys, :],
                send_sem=zs.at[0, j], recv_sem=zr.at[0, j], device_id=up, device_id_type=MESH)
        return pltpu.make_async_remote_copy(
            src_ref=f.at[pl.ds(0, RZ), ys, :], dst_ref=above.at[:, ys, :],
            send_sem=zs.at[1, j], recv_sem=zr.at[1, j], device_id=dn, device_id_type=MESH)

    def x_copy(side):
        if side == 0:
            return pltpu.make_async_remote_copy(
                src_ref=pack_r, dst_ref=got_l,
                send_sem=xs.at[0], recv_sem=xr.at[0], device_id=rt, device_id_type=MESH)
        return pltpu.make_async_remote_copy(
            src_ref=pack_l, dst_ref=got_r,
            send_sem=xs.at[1], recv_sem=xr.at[1], device_id=lf, device_id_type=MESH)

    for j in range(CHUNKS):
        @pl.when(has_up)
        def _():
            z_copy(0, j).start()

        @pl.when(has_dn)
        def _():
            z_copy(1, j).start()

    def bulk(k):
        da, dw = k // 2, k % 2
        ta, tw = lax.rem(c + da, 2), lax.rem(w + dw, 2)
        x0 = pl.multiple_of(LANES * slab_of(ta, tw), LANES)
        return pltpu.make_async_remote_copy(
            src_ref=chosen.at[:, :, pl.ds(x0, LANES)],
            dst_ref=moved.at[pl.ds(nb * c, nb), pl.ds(pl.multiple_of(ny * w, 8), ny), :],
            send_sem=bs.at[k], recv_sem=br.at[k],
            device_id=(4 * h + 2 * ta + a, tw), device_id_type=MESH)

    def bulk_wait():
        for k in range(4):
            if k:
                bulk(k).wait()
            else:
                @pl.when(c != a)
                def _():
                    bulk(0).wait()

    if kind < 3:
        fetch.wait()
        chosen[...] = stage[view[0]]

        @pl.when(c != a)
        def _():
            bulk(0).start()

        for k in range(1, 4):
            bulk(k).start()

        @pl.when(c == a)
        def _():
            x0 = pl.multiple_of(LANES * slab_of(c, w), LANES)
            moved[pl.ds(nb * c, nb), pl.ds(pl.multiple_of(ny * w, 8), ny), :] = chosen[:, :, pl.ds(x0, LANES)]

    @pl.when(jnp.logical_not(has_dn))
    def _():
        below[...] = jnp.zeros_like(below)

    @pl.when(jnp.logical_not(has_up))
    def _():
        above[...] = jnp.zeros_like(above)

    @pl.when(jnp.logical_not(has_l))
    def _():
        got_l[...] = jnp.zeros_like(got_l)

    @pl.when(jnp.logical_not(has_r))
    def _():
        got_r[...] = jnp.zeros_like(got_r)

    half = 16

    def z_tile(t, carry):
        ys = pl.ds(pl.multiple_of(8 * t, 8), 8)
        taps = [wz[k] for k in range(2 * RZ + 1)]
        for first in range(0, planes, half):
            acc = [None] * half
            for p in range(first, first + half + 2 * RZ):
                if p < RZ:
                    v = below[p, ys, :]
                elif p < RZ + planes:
                    v = f[p - RZ, ys, :]
                else:
                    v = above[p - RZ - planes, ys, :]
                for o in range(half):
                    k = p - first - o
                    if 0 <= k <= 2 * RZ:
                        term = taps[k] * v
                        acc[o] = term if acc[o] is None else acc[o] + term
            for o in range(half):
                zb[first + o, ys, :] = acc[o]
        return carry

    for j in range(CHUNKS):
        @pl.when(has_dn)
        def _():
            z_copy(0, j).wait_recv()

        @pl.when(has_up)
        def _():
            z_copy(1, j).wait_recv()

        lax.fori_loop(j * part // 8, (j + 1) * part // 8, z_tile, 0)

    for j in range(CHUNKS):
        @pl.when(has_up)
        def _():
            z_copy(0, j).wait_send()

        @pl.when(has_dn)
        def _():
            z_copy(1, j).wait_send()

    lane = lax.broadcasted_iota(jnp.int32, (rows, LANES), 1)
    per = LANES // 8

    for q in range(planes // per):
        packed_l = packed_r = None
        for k in range(0, per, 2):
            p = q * per + k
            his, los = zip(*(split(zb[p + i]) for i in range(2)))
            hi = jnp.concatenate(his, axis=1)
            lo = jnp.concatenate(los, axis=1)
            got = jnp.dot(ym[...], jnp.concatenate([hi, lo, hi, lo], axis=0),
                          preferred_element_type=jnp.float32)
            for i in range(2):
                value = got[:, i * LANES:(i + 1) * LANES]
                zb[p + i] = value
                at = 8 * (k + i)
                left = value if at == 0 else pltpu.roll(value, at, 1)
                right = pltpu.roll(value, (at + 8) % LANES, 1) if at + 8 < LANES else value
                if packed_l is None:
                    packed_l, packed_r = left, right
                else:
                    packed_l = jnp.where(lane >= at, left, packed_l)
                    packed_r = jnp.where(lane >= at, right, packed_r)
        pack_l[q] = packed_l
        pack_r[q] = packed_r

    @pl.when(has_r)
    def _():
        x_copy(0).start()

    @pl.when(has_l)
    def _():
        x_copy(1).start()

    step = 4
    for p in range(0, planes, step):
        hi, lo = split(zb[p:p + step].reshape(step * rows, LANES))
        got = jnp.dot(jnp.concatenate([hi, lo], axis=1), xm[...], preferred_element_type=jnp.float32)
        zb[p:p + step] = (got[:, :LANES] + got[:, LANES:]).reshape(step, rows, LANES)

    @pl.when(has_l)
    def _():
        x_copy(0).wait_recv()

    @pl.when(has_r)
    def _():
        x_copy(1).wait_recv()

    if divide:
        bulk_wait()

    for p in range(0, planes, step):
        edges = []
        for i in range(step):
            q, k = divmod(p + i, per)
            left, right = got_l[q], got_r[q]
            at = 8 * k
            left = left if at == 0 else pltpu.roll(left, LANES - at, 1)
            right = right if at == 8 else pltpu.roll(right, (LANES - at + 8) % LANES, 1)
            edges.append(jnp.where(lane < 8, left, right))
        hi, lo = split(jnp.concatenate(edges, axis=0))
        got = jnp.dot(jnp.concatenate([hi, lo], axis=1), xe[...], preferred_element_type=jnp.float32)
        value = zb[p:p + step] + (got[:, :LANES] + got[:, LANES:]).reshape(step, rows, LANES)
        if kind == 0:
            out[p:p + step] = moved[p:p + step] / value
        elif kind == 2:
            block, within = divmod(p, nz)
            held = other if within < nb else moved
            at = block * nb + within % nb
            out[p:p + step] = held[at:at + step] / value
        else:
            out[p:p + step] = other[p:p + step] * value

    @pl.when(has_r)
    def _():
        x_copy(0).wait_send()

    @pl.when(has_l)
    def _():
        x_copy(1).wait_send()

    if kind == 1:
        bulk_wait()


def slab_blur(kind, chain, f, other, weights, view, measured):
    planes, rows, _ = f.shape
    vmem = pl.BlockSpec(memory_space=pltpu.VMEM)
    packs = pltpu.VMEM((planes * 8 // LANES, rows, LANES), jnp.float32)
    like = jax.ShapeDtypeStruct
    args = [f] + ([other] if kind else []) + list(weights)
    in_specs = [vmem] * len(args)
    out_shape = [like(f.shape, jnp.float32)]
    scratch = [
        pltpu.VMEM((RZ, rows, LANES), jnp.float32),
        pltpu.VMEM((RZ, rows, LANES), jnp.float32),
        pltpu.VMEM((planes, rows, LANES), jnp.float32),
        packs, packs, packs, packs,
        pltpu.SemaphoreType.DMA((2, CHUNKS)),
        pltpu.SemaphoreType.DMA((2, CHUNKS)),
        pltpu.SemaphoreType.DMA((2,)),
        pltpu.SemaphoreType.DMA((2,)),
    ]
    if kind < 3:
        views, nz, ny, nx = measured.shape
        nb = nz if kind == 0 else nz // 2
        args += [view, measured]
        in_specs += [pl.BlockSpec(memory_space=pltpu.SMEM), pl.BlockSpec(memory_space=pl.ANY)]
        scratch += [
            pltpu.VMEM((views, nb, ny, nx), jnp.float32),
            pltpu.VMEM((nb, ny, nx), jnp.float32),
            pltpu.SemaphoreType.DMA((4,)),
            pltpu.SemaphoreType.DMA((4,)),
            pltpu.SemaphoreType.DMA,
        ]
        if kind == 1:
            out_shape.append(like((2 * nb, rows, LANES), jnp.float32))
        else:
            scratch.append(pltpu.VMEM((2 * nb, rows, LANES), jnp.float32))
    out = pl.pallas_call(
        functools.partial(blur_kernel, kind, chain),
        out_shape=out_shape,
        in_specs=in_specs,
        out_specs=[vmem] * len(out_shape),
        scratch_shapes=scratch,
        compiler_params=pltpu.CompilerParams(collective_id=3 + kind, has_side_effects=True),
    )(*args)
    return out


def slabs(chain, estimate, measured, psf_z, psf_y, psf_x, extents, order):
    views, nz, ny, nx = measured.shape
    current, weights = spread_first(estimate, psf_z, psf_y, psf_x, extents, order)
    seen = [order[p:p + 1] for p in range(views)]
    half = None
    for p in range(views):
        kind = 2 if p else 0
        ratio, = slab_blur(kind, chain, current, half, weights[2 * p], seen[p], measured)
        if p < views - 1:
            current, half = slab_blur(1, chain, ratio, current, weights[2 * p + 1], seen[p + 1], measured)
        else:
            current, = slab_blur(3, chain, ratio, current, weights[2 * p + 1], None, None)
    return gather_back(current, nz, ny, nx)


def on_device(estimate, measured, psf_z, psf_y, psf_x, extents, order):
    n_z, n_y = lax.axis_size("gz"), lax.axis_size("gy")
    nz, ny, nx = estimate.shape
    fits = n_y == 2 and n_z % 4 == 0 and nx == 4 * LANES and nz == 16 and 2 * ny == 64
    if fits:
        return slabs(n_z // 2, estimate, measured, psf_z, psf_y, psf_x, extents, order)
    return general(estimate, measured, psf_z, psf_y, psf_x, extents, order)


def solution(mesh):
    return jax.shard_map(
        on_device,
        mesh=mesh,
        in_specs=(P("gz", "gy", None), P(None, "gz", "gy", None), P(), P(), P(), P(), P()),
        out_specs=P("gz", "gy", None),
        check_vma=False,
    )
```
